32 devices in a mesh: seq: 8 (over y, x, core), tp: 4 (over z).
Axes of the slice: x: 2, y: 2, z: 4, core: 2. Of those that a mesh axis runs over, the one named last changes fastest.
Arguments:
- hidden: bfloat16 [8192, 2560], P('seq', 'tp'), may hold values from -6 to 6
- gate_proj: bfloat16 [2560, 5120], P(None, 'tp'), may hold values from -0.125 to 0.125
- input_proj: bfloat16 [2560, 5120], P(None, 'tp'), may hold values from -0.125 to 0.125
- bc_proj: bfloat16 [2560, 256], replicated, may hold values from -0.125 to 0.125
- step_proj: bfloat16 [2560, 80], P(None, 'tp'), may hold values from -0.125 to 0.125
- step_bias: float32 [80], P('tp'), may hold values from -16 to -3
- decay_log: float32 [80], P('tp'), may hold values from 0 to 2.78
- conv_weight: float32 [4, 5120], P(None, 'tp'), may hold values from -3 to 3
- conv_bias: float32 [5120], P('tp'), may hold values from -3 to 3
- bc_conv_weight: float32 [4, 256], replicated, may hold values from -3 to 3
- bc_conv_bias: float32 [256], replicated, may hold values from -3 to 3
- skip_gain: float32 [80], P('tp'), may hold values from 0.5 to 2
- norm_gain: float32 [5120], P('tp'), may hold values from 0.1 to 1.9
- out_proj: bfloat16 [5120, 2560], P('tp'), may hold values from -0.078125 to 0.078125
- amax_history: float32 [16], replicated, may hold values from 1.5 to 4
Outputs:
- mixed: bfloat16 [8192, 2560], P('seq', 'tp')
- new_history: float32 [16], replicated
The draws below stay inside these ranges and needn't reach their ends.
All inputs are finite; a program needn't handle non-finite values.
Results may differ from the reference program's by a relative error of at most 0.015.
Values may be sent and summed in bfloat16 or wider, within the bound.
A program may use at most 192 MiB of HBM per device.

```python
import math
import jax
import jax.numpy as jnp
from jax import lax

D = 2560
HEADS = 80
HEAD_DIM = 64
STATE = 128
CONV = 4
BLOCK = 256
HIST = 16
INNER = 5120
TOKENS = 8192


def head_rates(key):
    base_key = jax.random.fold_in(key, 7)
    key_rate, key_kind, key_slow, key_fast = jax.random.split(base_key, 4)
    decay_rate = jnp.exp(jax.random.uniform(key_rate, (HEADS,), jnp.float32, 0.0, math.log(16.0)))
    slow_share = 0.5
    slow_heads = jax.random.uniform(key_kind, (HEADS,), jnp.float32) < slow_share
    slow_rate = jax.random.uniform(key_slow, (HEADS,), jnp.float32, 0.3, 1.5) / TOKENS
    fast_rate = 1.0 / jax.random.uniform(key_fast, (HEADS,), jnp.float32, 30.0, 50.0)
    mean_rate = jnp.where(slow_heads, slow_rate, fast_rate)
    return (decay_rate, mean_rate / decay_rate)


def draw_decay_log(key, part):
    decay_rate, step_mean = head_rates(key)
    return jnp.log(decay_rate).astype(jnp.float32)


def draw_step_bias(key, part):
    decay_rate, step_mean = head_rates(key)
    return jnp.log(jnp.expm1(step_mean)).astype(jnp.float32)


def levels(key, extent, shards, least, largest):
    factor_of = 1.0
    for dim, blocks in shards:
        heights = jax.random.uniform(jax.random.fold_in(jax.random.fold_in(key, 6), dim), (blocks,), jnp.float32, least / len(shards), largest / len(shards))
        factor_of = factor_of * jnp.repeat(jnp.exp(heights), extent[dim] // blocks).reshape((-1,) + (1,) * (len(extent) - 1 - dim))
    return factor_of


def bell_draw(own_key, extent, width, most, cuts=(), kind=jnp.bfloat16):
    values = width * jax.random.normal(own_key, extent, jnp.float32)
    if cuts:
        values = values * levels(own_key, extent, cuts, -0.22, 0.18)
    return jnp.clip(values, -most, most).astype(kind)


def setup_inputs(seed: int = 0) -> dict:
    key_of = jax.random.split(jax.random.key(seed), 16)
    hidden = bell_draw(key_of[0], (TOKENS, D), 1.0, 6.0, ((0, 8), (1, 4)))
    gate_proj = bell_draw(key_of[1], (D, INNER), D ** -0.5, 0.125, ((1, 4),))
    input_proj = bell_draw(key_of[2], (D, INNER), D ** -0.5, 0.125, ((1, 4),))
    bc_proj = bell_draw(key_of[3], (D, 2 * STATE), D ** -0.5, 0.125)
    step_proj = bell_draw(key_of[4], (D, HEADS), D ** -0.5, 0.125, ((1, 4),))
    step_bias = draw_step_bias(jax.random.fold_in(key_of[15], 71), 0)
    decay_log = draw_decay_log(jax.random.fold_in(key_of[15], 71), 0)
    conv_weight = bell_draw(key_of[7], (CONV, INNER), CONV ** -0.5, 3.0, ((1, 4),), jnp.float32)
    conv_bias = bell_draw(key_of[8], (INNER,), 0.5, 3.0, ((0, 4),), jnp.float32)
    bc_conv_weight = bell_draw(key_of[9], (CONV, 2 * STATE), CONV ** -0.5, 3.0, (), jnp.float32)
    bc_conv_bias = bell_draw(key_of[10], (2 * STATE,), 0.5, 3.0, (), jnp.float32)
    skip_gain = jnp.clip(0.5 + 1.5 * jax.random.uniform(key_of[11], (HEADS,), jnp.float32) ** levels(key_of[11], (HEADS,), ((0, 4),), -0.2, 0.2), 0.5, 2.0)
    norm_gain = jnp.clip(1.0 + 0.18 * jax.random.normal(key_of[12], (INNER,), jnp.float32), 0.1, 1.9)
    out_proj = bell_draw(key_of[13], (INNER, D), INNER ** -0.5, 0.078125, ((0, 4),))
    amax_history = jnp.clip(jax.random.uniform(key_of[14], (HIST,), jnp.float32, 1.5, 4.0), 1.5, 4.0)
    return {"hidden": hidden, "gate_proj": gate_proj, "input_proj": input_proj, "bc_proj": bc_proj, "step_proj": step_proj, "step_bias": step_bias, "decay_log": decay_log, "conv_weight": conv_weight, "conv_bias": conv_bias, "bc_conv_weight": bc_conv_weight, "bc_conv_bias": bc_conv_bias, "skip_gain": skip_gain, "norm_gain": norm_gain, "out_proj": out_proj, "amax_history": amax_history}


QMAX = 448.0
EPS = 1e-05

def conv_silu(pre_conv, weight, conv_shift):
    row_count = pre_conv.shape[0]
    kernel = weight.shape[0]
    padded = jnp.concatenate([jnp.zeros((kernel - 1, pre_conv.shape[1]), jnp.bfloat16), pre_conv], axis=0)
    running = jnp.zeros(pre_conv.shape, jnp.float32)
    for offset in range(kernel):
        running = running + weight[offset] * padded[offset:offset + row_count].astype(jnp.float32)
    return jax.nn.silu(running + conv_shift).astype(jnp.bfloat16)

def ssd_block(carry_state, block_data):
    x_block, b_block, c_block, step_block, decay_block = block_data
    length = x_block.shape[0]
    head_count = carry_state.shape[0]
    head_width = carry_state.shape[1]
    cum_decay = jnp.cumsum(decay_block, axis=1)
    scores = jnp.dot(c_block, b_block.T, preferred_element_type=jnp.float32)
    causal = lax.broadcasted_iota(jnp.int32, (length, length), 0) >= lax.broadcasted_iota(jnp.int32, (length, length), 1)
    decay_gap = cum_decay[:, :, None] - cum_decay[:, None, :]
    decay_mask = jnp.where(causal, jnp.exp(jnp.where(causal, decay_gap, 0.0)), 0.0)
    weights = (scores[None] * decay_mask * step_block[:, None, :]).astype(jnp.bfloat16)
    x_heads = x_block.reshape(length, head_count, head_width)
    intra_out = jnp.einsum('hts,shp->htp', weights.astype(jnp.float32), x_heads.astype(jnp.float32))
    inter_out = jnp.exp(cum_decay)[:, :, None] * jnp.einsum('tn,hpn->htp', c_block.astype(jnp.float32), carry_state, precision=lax.Precision.HIGHEST)
    tail_decay = jnp.exp(cum_decay[:, -1:] - cum_decay) * step_block
    x_weighted = (tail_decay.T[:, :, None] * x_heads.astype(jnp.float32)).astype(jnp.bfloat16)
    update = jnp.einsum('shp,sn->hpn', x_weighted.astype(jnp.float32), b_block.astype(jnp.float32))
    next_state = jnp.exp(cum_decay[:, -1])[:, None, None] * carry_state + update
    block_out = (intra_out + inter_out).transpose(1, 0, 2).reshape(length, head_count * head_width)
    return (next_state, block_out)

def reference(hidden, gate_proj, input_proj, bc_proj, step_proj, step_bias, decay_log, conv_weight, conv_bias, bc_conv_weight, bc_conv_bias, skip_gain, norm_gain, out_proj, amax_history):
    gate_in = jnp.dot(hidden, gate_proj, preferred_element_type=jnp.float32).astype(jnp.bfloat16)
    x_pre = jnp.dot(hidden, input_proj, preferred_element_type=jnp.float32).astype(jnp.bfloat16)
    bc_pre = jnp.dot(hidden, bc_proj, preferred_element_type=jnp.float32).astype(jnp.bfloat16)
    step_raw = jnp.dot(hidden, step_proj, preferred_element_type=jnp.float32)
    x_conv = conv_silu(x_pre, conv_weight, conv_bias)
    bc_conv = conv_silu(bc_pre, bc_conv_weight, bc_conv_bias)
    b_in = bc_conv[:, :STATE]
    c_out = bc_conv[:, STATE:]
    step_size = jax.nn.softplus(step_raw + step_bias)
    log_decay = step_size * -jnp.exp(decay_log)
    blocks = TOKENS // BLOCK
    stacked = (x_conv.reshape(blocks, BLOCK, INNER), b_in.reshape(blocks, BLOCK, STATE), c_out.reshape(blocks, BLOCK, STATE), step_size.reshape(blocks, BLOCK, HEADS).transpose(0, 2, 1), log_decay.reshape(blocks, BLOCK, HEADS).transpose(0, 2, 1))
    start_state = jnp.zeros((HEADS, HEAD_DIM, STATE), jnp.float32)
    final_state, block_outs = lax.scan(ssd_block, start_state, stacked)
    ssm_out = block_outs.reshape(TOKENS, INNER)
    x_heads = x_conv.reshape(TOKENS, HEADS, HEAD_DIM).astype(jnp.float32)
    ssm_out = ssm_out + (skip_gain[:, None] * x_heads).reshape(TOKENS, INNER)
    gated = ssm_out * jax.nn.silu(gate_in.astype(jnp.float32))
    inv_rms = lax.rsqrt(lax.optimization_barrier(jnp.mean(gated * gated, axis=1)) + EPS)
    normed = gated * inv_rms[:, None] * norm_gain
    peak_value = jnp.max(jnp.abs(normed))
    scale = QMAX / jnp.max(amax_history)
    quant = jnp.clip(normed * scale, -QMAX, QMAX).astype(jnp.bfloat16)
    mixed = (jnp.dot(quant, out_proj, preferred_element_type=jnp.float32) / scale).astype(jnp.bfloat16)
    new_history = jnp.concatenate([peak_value.reshape(1), amax_history[:-1]])
    return (mixed, new_history)
```

```python
import functools

import jax
import jax.numpy as jnp
from jax import lax
from jax.experimental import pallas as pl
from jax.experimental.pallas import tpu as pltpu
from jax.sharding import PartitionSpec as P

BLOCK = 256
QMAX = 448.0
EPS = 1e-05
LANES = 128
F32 = jnp.float32
BF16 = jnp.bfloat16
GATHER_PARTS = (3, 1)
OUT_PARTS = (1, 3)
VMEM = 60 * 1024 * 1024


def conv_silu(padded, row_count, weight, conv_shift):
    kernel = weight.shape[0]
    running = jnp.zeros((row_count, padded.shape[1]), F32)
    for offset in range(kernel):
        running = running + weight[offset] * padded[offset : offset + row_count].astype(F32)
    return jax.nn.silu(running + conv_shift).astype(BF16)


def spread(lane, cols):
    out = cols[0]
    for i in range(1, len(cols)):
        out = jnp.where(lane < i, out, cols[i])
    return out


def lane_head(rows, width):
    return lax.broadcasted_iota(jnp.int32, (rows, LANES), 1) // width


def ssd_kernel(
    width, x_ref, b_ref, c_ref, step_ref, rate_ref, skip_ref, held_ref, sum_ref,
    y_ref, u_ref, cum_ref, local_ref, total_ref,
):
    length = x_ref.shape[0]
    group = LANES // width
    row = lax.broadcasted_iota(jnp.int32, (length, length), 0)
    col = lax.broadcasted_iota(jnp.int32, (length, length), 1)
    causal = row >= col
    ones = jnp.where(causal, 1.0, 0.0).astype(F32)
    step = step_ref[...]
    decay = step * rate_ref[...]
    cum = jnp.dot(ones, decay, precision=lax.Precision.HIGHEST, preferred_element_type=F32)
    cum_ref[...] = cum
    tail = jnp.exp(jnp.minimum(cum[length - 1 :, :] - cum, 0.0)) * step
    cum_t = cum.T
    step_t = step.T
    b = b_ref[...]
    scores = lax.dot_general(c_ref[...], b, (((1,), (1,)), ((), ())), preferred_element_type=F32)
    scores = jnp.where(causal, scores, 0.0)
    lane = lane_head(length, width)
    for p in range(x_ref.shape[1] // LANES):
        sl = slice(p * LANES, (p + 1) * LANES)
        xp = x_ref[:, sl]
        heads = range(p * group, (p + 1) * group)
        ys = []
        for h in heads:
            gap = jnp.minimum(cum[:, h : h + 1] - cum_t[h : h + 1, :], 0.0)
            w = (scores * jnp.exp(gap) * step_t[h : h + 1, :]).astype(BF16)
            ys.append(jnp.dot(w, xp, preferred_element_type=F32))
        xf = xp.astype(F32)
        y = spread(lane, ys) + skip_ref[:, sl] * xf
        y_ref[:, sl] = y.astype(y_ref.dtype)
        tail_p = spread(lane, [tail[:, h : h + 1] for h in heads])
        xw = (tail_p * xf).astype(BF16)
        update = lax.dot_general(b, xw, (((0,), (0,)), ((), ())), preferred_element_type=F32)
        u_ref[:, sl] = update
        last = spread(lane[:1], [cum[length - 1 :, h : h + 1] for h in heads])
        local_ref[:, sl] = jnp.exp(last) * held_ref[:, sl] + update
        total_ref[:, sl] = sum_ref[:, sl] + last


def ssd_chunk(x, b, c, step, rate, skip, held, total, width):
    length, inner = x.shape
    state = b.shape[1]
    return pl.pallas_call(
        functools.partial(ssd_kernel, width),
        out_shape=(
            jax.ShapeDtypeStruct((length, inner), BF16),
            jax.ShapeDtypeStruct((state, inner), F32),
            jax.ShapeDtypeStruct((length, LANES), F32),
            jax.ShapeDtypeStruct((state, inner), F32),
            jax.ShapeDtypeStruct((1, inner), F32),
        ),
        cost_estimate=pl.CostEstimate(
            flops=4 * length * length * inner, bytes_accessed=8 * length * inner, transcendentals=length * length * inner // width
        ),
        compiler_params=pltpu.CompilerParams(vmem_limit_bytes=VMEM),
        name="ssd_chunk",
    )(x, b, c, step, rate, skip, held, total)


def gate_kernel(width, y_ref, gate_ref, c_ref, cum_ref, u_ref, in_ref, gain_ref, o_ref, sq_ref, mx_ref, state):
    length = y_ref.shape[0]
    group = LANES // width

    @pl.when(pl.program_id(0) == 0)
    def _():
        state[...] = in_ref[...]

    reach = jnp.exp(cum_ref[...])
    c = c_ref[...]
    lane = lane_head(length, width)
    total = jnp.zeros((length, LANES), F32)
    most = jnp.zeros((length, LANES), F32)
    for p in range(y_ref.shape[1] // LANES):
        sl = slice(p * LANES, (p + 1) * LANES)
        held = state[:, sl]
        inter = jnp.dot(c, held.astype(BF16), preferred_element_type=F32)
        reach_p = spread(lane, [reach[:, h : h + 1] for h in range(p * group, (p + 1) * group)])
        g = gate_ref[:, sl].astype(F32)
        gated = (y_ref[:, sl].astype(F32) + reach_p * inter) * (g / (1.0 + jnp.exp(-g)))
        o_ref[:, sl] = gated.astype(o_ref.dtype)
        total = total + gated * gated
        most = jnp.maximum(most, jnp.abs(gated * gain_ref[:, sl]))
        state[:, sl] = reach_p[length - 1 :, :] * held + u_ref[:, sl]
    sq_ref[...] = jnp.sum(total, axis=1, keepdims=True)
    mx_ref[...] = jnp.max(most, axis=1, keepdims=True)


def gate_all(y, gate, c, cum, u, incoming, gain, width):
    rows, inner = y.shape
    n = c.shape[1]
    tile = lambda h, w: pl.BlockSpec((h, w), lambda i: (i, 0))
    whole = lambda h, w: pl.BlockSpec((h, w), lambda i: (0, 0))
    return pl.pallas_call(
        functools.partial(gate_kernel, width),
        grid=(rows // BLOCK,),
        in_specs=[
            tile(BLOCK, inner), tile(BLOCK, inner), tile(BLOCK, n), tile(BLOCK, LANES), tile(n, inner),
            whole(n, inner), whole(1, inner),
        ],
        out_specs=(tile(BLOCK, inner), tile(BLOCK, 1), tile(BLOCK, 1)),
        out_shape=(
            jax.ShapeDtypeStruct((rows, inner), BF16),
            jax.ShapeDtypeStruct((rows, 1), F32),
            jax.ShapeDtypeStruct((rows, 1), F32),
        ),
        scratch_shapes=[pltpu.VMEM((n, inner), F32)],
        compiler_params=pltpu.CompilerParams(vmem_limit_bytes=VMEM),
        cost_estimate=pl.CostEstimate(
            flops=2 * rows * inner * n, bytes_accessed=8 * rows * inner, transcendentals=rows * inner
        ),
        name="gate_all",
    )(y, gate, c, cum, u, incoming, gain)


def out_kernel(gated_ref, inv_ref, gain_ref, w_ref, o_ref, quant):
    @pl.when(pl.program_id(0) == 0)
    def _():
        v = gated_ref[...].astype(F32) * inv_ref[...] * gain_ref[...]
        quant[...] = jnp.clip(v, -QMAX, QMAX).astype(BF16)

    o_ref[0] = jnp.dot(quant[...], w_ref[...], preferred_element_type=F32).astype(BF16)


def out_part(gated, inv, gain, w, first, count, places):
    inner, model = w.shape
    width = model // places
    rows = count * BLOCK
    gated, inv = gated[first * BLOCK :][:rows], inv[first * BLOCK :][:rows]
    return pl.pallas_call(
        out_kernel,
        grid=(places,),
        in_specs=[
            pl.BlockSpec((rows, inner), lambda i: (0, 0)),
            pl.BlockSpec((rows, 1), lambda i: (0, 0)),
            pl.BlockSpec((1, inner), lambda i: (0, 0)),
            pl.BlockSpec((inner, width), lambda i: (0, i)),
        ],
        out_specs=pl.BlockSpec((1, rows, width), lambda i: (i, 0, 0)),
        out_shape=jax.ShapeDtypeStruct((places, rows, width), BF16),
        scratch_shapes=[pltpu.VMEM((rows, inner), BF16)],
        compiler_params=pltpu.CompilerParams(vmem_limit_bytes=VMEM),
        cost_estimate=pl.CostEstimate(
            flops=2 * rows * inner * model, bytes_accessed=2 * inner * model, transcendentals=0
        ),
        name="out_part",
    )(gated, inv, gain, w)


def incoming_state(local, decay_row):
    place = lax.axis_index("seq")
    size = lax.axis_size("seq")
    high = decay_row.astype(BF16)
    low = (decay_row - high.astype(F32)).astype(BF16)
    pad = jnp.zeros((14, local.shape[1]), BF16)
    packed = jnp.concatenate([local.astype(BF16), high, low, pad], axis=0)
    every = lax.all_gather(packed, "seq")
    n = local.shape[0]
    decays = every[:, n].astype(F32) + every[:, n + 1].astype(F32)
    j = jnp.arange(size)
    between = (j[:, None] < j[None, :]) & (j[None, :] < place)
    gaps = jnp.sum(jnp.where(between[:, :, None], decays[None], 0.0), axis=1)
    weight = jnp.where((j < place)[:, None], jnp.exp(gaps), 0.0)
    return jnp.sum(weight[:, None, :] * every[:, :n].astype(F32), axis=0)


def shards(
    hidden, gate_proj, input_proj, bc_proj, step_proj, step_bias, decay_log, conv_weight, conv_bias,
    bc_conv_weight, bc_conv_bias, skip_gain, norm_gain, out_proj, amax_history,
):
    rows = hidden.shape[0]
    inner = gate_proj.shape[1]
    n = bc_proj.shape[1] // 2
    heads = step_proj.shape[1]
    width = inner // heads
    keep = conv_weight.shape[0] - 1
    places = lax.axis_size("tp")
    blocks = rows // BLOCK
    halo = 16
    size = lax.axis_size("seq")
    rim_hidden = lax.ppermute(hidden[rows - halo :], "seq", [(i, i + 1) for i in range(size - 1)])
    parts = GATHER_PARTS if sum(GATHER_PARTS) == blocks else (1,) * blocks
    turn = 0
    fill = LANES - heads
    step_weight = jnp.pad(step_proj, ((0, 0), (0, fill)))
    step_shift = jnp.pad(step_bias, (0, fill))
    rate = jnp.pad(-jnp.exp(decay_log), (0, fill))[None]
    skip_row = jnp.repeat(skip_gain, width)[None]
    join = lambda pieces: jnp.concatenate(pieces, axis=0)
    pieces = []
    at = 0
    for i, count in enumerate(parts):
        own = hidden[at * BLOCK : (at + count) * BLOCK]
        at += count
        if i == turn:
            own = join([rim_hidden, own])
        else:
            own, pieces[-1] = lax.optimization_barrier((own, pieces[-1]))
        pieces.append(lax.all_gather(own, "tp", axis=1, tiled=True))
    gates, ys, us, cums, cs = [], [], [], [], []
    local = jnp.zeros((n, inner), F32)
    total = jnp.zeros((1, inner), F32)
    raw_x, raw_bc, steps = [], [], []
    for i, count in enumerate(parts):
        piece = pieces[i]
        x_raw = jnp.dot(piece, input_proj, preferred_element_type=F32).astype(BF16)
        bc_raw = jnp.dot(piece, bc_proj, preferred_element_type=F32).astype(BF16)
        if i == turn:
            rim = (x_raw[halo - keep : halo], bc_raw[halo - keep : halo])
            x_raw, bc_raw, piece = x_raw[halo:], bc_raw[halo:], piece[halo:]
        raw_x.append(x_raw)
        raw_bc.append(bc_raw)
        steps.append(jax.nn.softplus(jnp.dot(piece, step_weight, preferred_element_type=F32) + step_shift))
        gates.append(jnp.dot(piece, gate_proj, preferred_element_type=F32).astype(BF16))
    for i, count in enumerate(parts):
        before = rim if i == 0 else (raw_x[i - 1][-keep:], raw_bc[i - 1][-keep:])
        x_all = conv_silu(join([before[0], raw_x[i]]), count * BLOCK, conv_weight, conv_bias)
        bc_all = conv_silu(join([before[1], raw_bc[i]]), count * BLOCK, bc_conv_weight, bc_conv_bias)
        for k in range(count):
            rows_k = slice(k * BLOCK, (k + 1) * BLOCK)
            x, bc = x_all[rows_k], bc_all[rows_k]
            b, c = bc[:, :n], bc[:, n:]
            y, u, cum, local, total = ssd_chunk(
                x, b, c, steps[i][rows_k], rate, skip_row, local, total, width
            )
            ys.append(y)
            us.append(u)
            cums.append(cum)
            cs.append(c)
    incoming = incoming_state(local, total)
    gated, squares, most = gate_all(
        join(ys), join(gates), join(cs), join(cums), join(us), incoming, norm_gain[None], width
    )
    squares = lax.psum(squares[:, 0], "tp")
    inv = lax.rsqrt(squares / (inner * places) + EPS)
    peak = jnp.max(most[:, 0] * inv)
    scale = QMAX / jnp.max(amax_history)
    gain_row = norm_gain[None] * scale
    results = []
    out_parts = OUT_PARTS if sum(OUT_PARTS) == blocks else (1,) * blocks
    at = 0
    for part, count in enumerate(out_parts):
        share = out_part(gated, inv[:, None], gain_row, out_proj, at, count, places)
        at += count
        if part == len(out_parts) - 1:
            share, peak = lax.optimization_barrier((share, peak))
        summed = lax.psum_scatter(share, "tp", scatter_dimension=0, tiled=False)
        results.append((summed.astype(F32) / scale).astype(BF16))
    peak = lax.pmax(peak, ("seq", "tp"))
    mixed = join(results)
    return (mixed, jnp.concatenate([jnp.reshape(peak, (1,)), amax_history[:-1]]))


def solution(mesh):
    return jax.shard_map(
        shards,
        mesh=mesh,
        in_specs=(
            P("seq", "tp"), P(None, "tp"), P(None, "tp"), P(), P(None, "tp"), P("tp"), P("tp"), P(None, "tp"),
            P("tp"), P(), P(), P("tp"), P("tp"), P("tp", None), P(),
        ),
        out_specs=(P("seq", "tp"), P()),
        check_vma=False,
    )
```

```python
import functools

import jax
import jax.numpy as jnp
from jax import lax
from jax.experimental import pallas as pl
from jax.experimental.pallas import tpu as pltpu
from jax.sharding import PartitionSpec as P

BLOCK = 256
QMAX = 448.0
EPS = 1e-05
LANES = 128
F32 = jnp.float32
BF16 = jnp.bfloat16
GATHER_PARTS = (3, 1)
OUT_PARTS = (1, 3)
VMEM = 56 * 1024 * 1024


def conv_silu(padded, row_count, weight, conv_shift):
    kernel = weight.shape[0]
    running = jnp.zeros((row_count, padded.shape[1]), F32)
    for offset in range(kernel):
        running = running + weight[offset] * padded[offset : offset + row_count].astype(F32)
    return jax.nn.silu(running + conv_shift).astype(BF16)


def spread(lane, cols):
    out = cols[0]
    for i in range(1, len(cols)):
        out = jnp.where(lane < i, out, cols[i])
    return out


def lane_head(rows, width):
    return lax.broadcasted_iota(jnp.int32, (rows, LANES), 1) // width


def ssd_kernel(
    width, x_ref, b_ref, c_ref, step_ref, rate_ref, skip_ref, held_ref, sum_ref,
    y_ref, u_ref, cum_ref, local_ref, total_ref,
):
    length = x_ref.shape[0]
    group = LANES // width
    row = lax.broadcasted_iota(jnp.int32, (length, length), 0)
    col = lax.broadcasted_iota(jnp.int32, (length, length), 1)
    causal = row >= col
    ones = jnp.where(causal, 1.0, 0.0).astype(F32)
    step = step_ref[...]
    decay = step * rate_ref[...]
    cum = jnp.dot(ones, decay, precision=lax.Precision.HIGHEST, preferred_element_type=F32)
    cum_ref[...] = cum
    tail = jnp.exp(jnp.minimum(cum[length - 1 :, :] - cum, 0.0)) * step
    cum_t = cum.T
    step_t = step.T
    b = b_ref[...]
    scores = lax.dot_general(c_ref[...], b, (((1,), (1,)), ((), ())), preferred_element_type=F32)
    scores = jnp.where(causal, scores, 0.0)
    lane = lane_head(length, width)
    for p in range(x_ref.shape[1] // LANES):
        sl = slice(p * LANES, (p + 1) * LANES)
        xp = x_ref[:, sl]
        heads = range(p * group, (p + 1) * group)
        ys = []
        for h in heads:
            gap = jnp.minimum(cum[:, h : h + 1] - cum_t[h : h + 1, :], 0.0)
            w = (scores * jnp.exp(gap) * step_t[h : h + 1, :]).astype(BF16)
            ys.append(jnp.dot(w, xp, preferred_element_type=F32))
        xf = xp.astype(F32)
        y = spread(lane, ys) + skip_ref[:, sl] * xf
        y_ref[:, sl] = y.astype(y_ref.dtype)
        tail_p = spread(lane, [tail[:, h : h + 1] for h in heads])
        xw = (tail_p * xf).astype(BF16)
        update = lax.dot_general(b, xw, (((0,), (0,)), ((), ())), preferred_element_type=F32)
        u_ref[:, sl] = update
        last = spread(lane[:1], [cum[length - 1 :, h : h + 1] for h in heads])
        local_ref[:, sl] = jnp.exp(last) * held_ref[:, sl] + update
        total_ref[:, sl] = sum_ref[:, sl] + last


def ssd_chunk(x, b, c, step, rate, skip, held, total, width):
    length, inner = x.shape
    state = b.shape[1]
    return pl.pallas_call(
        functools.partial(ssd_kernel, width),
        out_shape=(
            jax.ShapeDtypeStruct((length, inner), BF16),
            jax.ShapeDtypeStruct((state, inner), F32),
            jax.ShapeDtypeStruct((length, LANES), F32),
            jax.ShapeDtypeStruct((state, inner), F32),
            jax.ShapeDtypeStruct((1, inner), F32),
        ),
        cost_estimate=pl.CostEstimate(
            flops=4 * length * length * inner, bytes_accessed=8 * length * inner, transcendentals=length * length * inner // width
        ),
        compiler_params=pltpu.CompilerParams(vmem_limit_bytes=VMEM),
        name="ssd_chunk",
    )(x, b, c, step, rate, skip, held, total)


def gate_kernel(width, blocks, gate_at, out_at, names, *refs):
    refs = dict(zip(names, refs))
    places = lax.axis_size("tp")
    me = lax.axis_index("tp")
    barrier = pltpu.get_barrier_semaphore()
    for k in range(1, places):
        pl.semaphore_signal(
            barrier, inc=1, device_id={"tp": lax.rem(me + k, places)}, device_id_type=pl.DeviceIdType.MESH
        )
    state, own, land, most_all = refs["state"], refs["own"], refs["land"], refs["most"]
    inner = state.shape[1]
    group = LANES // width
    state[...] = refs["incoming"][...]
    own[...] = jnp.zeros_like(own)
    lane = lane_head(BLOCK, width)
    for i in range(blocks):
        g_name, g_row = gate_at[i]
        o_name, o_row = out_at[i]
        reach = jnp.exp(refs["cum%d" % i][...])
        c = refs["c%d" % i][...]
        total = jnp.zeros((BLOCK, LANES), F32)
        most = jnp.zeros((BLOCK, LANES), F32)
        for p in range(inner // LANES):
            sl = slice(p * LANES, (p + 1) * LANES)
            held = state[:, sl]
            inter = jnp.dot(c, held.astype(BF16), preferred_element_type=F32)
            reach_p = spread(lane, [reach[:, h : h + 1] for h in range(p * group, (p + 1) * group)])
            g = refs[g_name][g_row : g_row + BLOCK, sl].astype(F32)
            y = refs["y%d" % i][:, sl].astype(F32)
            gated = (y + reach_p * inter) * (g / (1.0 + jnp.exp(-g)))
            refs[o_name][o_row : o_row + BLOCK, sl] = gated.astype(BF16)
            total = total + gated * gated
            most = jnp.maximum(most, jnp.abs(gated * refs["gain"][:, sl]))
            state[:, sl] = reach_p[BLOCK - 1 :, :] * held + refs["u%d" % i][:, sl]
        own[i : i + 1, :] = jnp.sum(total.T, axis=0, keepdims=True)
        most_all[i] = most
    pl.semaphore_wait(barrier, places - 1)
    copies = []
    for k in range(1, places):
        copies.append(
            pltpu.make_async_remote_copy(
                src_ref=own,
                dst_ref=land.at[k - 1],
                send_sem=refs["send"].at[k - 1],
                recv_sem=refs["recv"].at[k - 1],
                device_id={"tp": lax.rem(me + k, places)},
                device_id_type=pl.DeviceIdType.MESH,
            )
        )
        copies[-1].start()
    for copy in copies:
        copy.wait()
    squares = own[...]
    for k in range(1, places):
        squares = squares + land[k - 1]
    inv = lax.rsqrt(squares / (inner * places) + EPS)
    peak = jnp.zeros((BLOCK, LANES), F32)
    for i in range(blocks):
        o_name, o_row = out_at[i]
        col = jnp.broadcast_to(inv[i : i + 1, :], (LANES, BLOCK)).T
        peak = jnp.maximum(peak, most_all[i] * col)
        for p in range(inner // LANES):
            sl = slice(p * LANES, (p + 1) * LANES)
            v = refs[o_name][o_row : o_row + BLOCK, sl].astype(F32) * col * refs["scaled"][:, sl]
            refs[o_name][o_row : o_row + BLOCK, sl] = jnp.clip(v, -QMAX, QMAX).astype(BF16)
    refs["peak"][...] = jnp.max(peak, axis=0, keepdims=True)


def gate_norm(ys, gates, cs, cums, us, incoming, gain, scaled, out_parts, width):
    blocks = len(ys)
    inner = ys[0].shape[1]
    n = cs[0].shape[1]
    places = lax.axis_size("tp")
    gate_at, out_at = [], []
    for i, piece in enumerate(gates):
        gate_at += [("gate%d" % i, k * BLOCK) for k in range(piece.shape[0] // BLOCK)]
    for i, count in enumerate(out_parts):
        out_at += [("quant%d" % i, k * BLOCK) for k in range(count)]
    ins = {}
    for name, group in (("y", ys), ("gate", gates), ("c", cs), ("cum", cums), ("u", us)):
        for i, a in enumerate(group):
            ins["%s%d" % (name, i)] = a
    ins.update(incoming=incoming, gain=gain, scaled=scaled)
    outs = {"quant%d" % i: jax.ShapeDtypeStruct((k * BLOCK, inner), BF16) for i, k in enumerate(out_parts)}
    outs["peak"] = jax.ShapeDtypeStruct((1, LANES), F32)
    deep = -(-blocks // 8) * 8
    scratch = {
        "state": pltpu.VMEM((n, inner), F32),
        "own": pltpu.VMEM((deep, BLOCK), F32),
        "land": pltpu.VMEM((places - 1, deep, BLOCK), F32),
        "most": pltpu.VMEM((blocks, BLOCK, LANES), F32),
        "send": pltpu.SemaphoreType.DMA((places - 1,)),
        "recv": pltpu.SemaphoreType.DMA((places - 1,)),
    }
    names = list(ins) + list(outs) + list(scratch)
    rows = blocks * BLOCK
    found = pl.pallas_call(
        functools.partial(gate_kernel, width, blocks, gate_at, out_at, names),
        in_specs=[pl.BlockSpec(memory_space=pltpu.VMEM)] * len(ins),
        out_specs=[pl.BlockSpec(memory_space=pltpu.VMEM)] * len(outs),
        out_shape=list(outs.values()),
        scratch_shapes=list(scratch.values()),
        compiler_params=pltpu.CompilerParams(vmem_limit_bytes=VMEM, collective_id=0, has_side_effects=True),
        cost_estimate=pl.CostEstimate(
            flops=2 * rows * inner * n, bytes_accessed=8 * rows * inner, transcendentals=rows * inner
        ),
        name="gate_norm",
    )(*ins.values())
    return found[:-1], jnp.max(found[-1])


def out_kernel(quant_ref, w_ref, o_ref):
    o_ref[0] = jnp.dot(quant_ref[...], w_ref[...], preferred_element_type=F32).astype(BF16)


def out_part(quant, w, places):
    rows, inner = quant.shape
    model = w.shape[1]
    width = model // places
    return pl.pallas_call(
        out_kernel,
        grid=(places,),
        in_specs=[
            pl.BlockSpec((rows, inner), lambda i: (0, 0)),
            pl.BlockSpec((inner, width), lambda i: (0, i)),
        ],
        out_specs=pl.BlockSpec((1, rows, width), lambda i: (i, 0, 0)),
        out_shape=jax.ShapeDtypeStruct((places, rows, width), BF16),
        compiler_params=pltpu.CompilerParams(vmem_limit_bytes=VMEM),
        cost_estimate=pl.CostEstimate(
            flops=2 * rows * inner * model, bytes_accessed=2 * inner * model, transcendentals=0
        ),
        name="out_part",
    )(quant, w)


def incoming_state(local, decay_row):
    place = lax.axis_index("seq")
    size = lax.axis_size("seq")
    high = decay_row.astype(BF16)
    low = (decay_row - high.astype(F32)).astype(BF16)
    pad = jnp.zeros((14, local.shape[1]), BF16)
    packed = jnp.concatenate([local.astype(BF16), high, low, pad], axis=0)
    every = lax.all_gather(packed, "seq")
    n = local.shape[0]
    decays = every[:, n].astype(F32) + every[:, n + 1].astype(F32)
    j = jnp.arange(size)
    between = (j[:, None] < j[None, :]) & (j[None, :] < place)
    gaps = jnp.sum(jnp.where(between[:, :, None], decays[None], 0.0), axis=1)
    weight = jnp.where((j < place)[:, None], jnp.exp(gaps), 0.0)
    return jnp.sum(weight[:, None, :] * every[:, :n].astype(F32), axis=0)


def shards(
    hidden, gate_proj, input_proj, bc_proj, step_proj, step_bias, decay_log, conv_weight, conv_bias,
    bc_conv_weight, bc_conv_bias, skip_gain, norm_gain, out_proj, amax_history,
):
    rows = hidden.shape[0]
    inner = gate_proj.shape[1]
    n = bc_proj.shape[1] // 2
    heads = step_proj.shape[1]
    width = inner // heads
    keep = conv_weight.shape[0] - 1
    places = lax.axis_size("tp")
    blocks = rows // BLOCK
    halo = 16
    size = lax.axis_size("seq")
    rim_hidden = lax.ppermute(hidden[rows - halo :], "seq", [(i, i + 1) for i in range(size - 1)])
    parts = GATHER_PARTS if sum(GATHER_PARTS) == blocks else (1,) * blocks
    turn = 0
    fill = LANES - heads
    step_weight = jnp.pad(step_proj, ((0, 0), (0, fill)))
    step_shift = jnp.pad(step_bias, (0, fill))
    rate = jnp.pad(-jnp.exp(decay_log), (0, fill))[None]
    skip_row = jnp.repeat(skip_gain, width)[None]
    join = lambda pieces: jnp.concatenate(pieces, axis=0)
    pieces = []
    at = 0
    for i, count in enumerate(parts):
        own = hidden[at * BLOCK : (at + count) * BLOCK]
        at += count
        if i == turn:
            own = join([rim_hidden, own])
        else:
            own, pieces[-1] = lax.optimization_barrier((own, pieces[-1]))
        pieces.append(lax.all_gather(own, "tp", axis=1, tiled=True))
    gates, ys, us, cums, cs = [], [], [], [], []
    local = jnp.zeros((n, inner), F32)
    total = jnp.zeros((1, inner), F32)
    raw_x, raw_bc, steps = [], [], []
    for i, count in enumerate(parts):
        piece = pieces[i]
        x_raw = jnp.dot(piece, input_proj, preferred_element_type=F32).astype(BF16)
        bc_raw = jnp.dot(piece, bc_proj, preferred_element_type=F32).astype(BF16)
        if i == turn:
            rim = (x_raw[halo - keep : halo], bc_raw[halo - keep : halo])
            x_raw, bc_raw, piece = x_raw[halo:], bc_raw[halo:], piece[halo:]
        raw_x.append(x_raw)
        raw_bc.append(bc_raw)
        steps.append(jax.nn.softplus(jnp.dot(piece, step_weight, preferred_element_type=F32) + step_shift))
        gates.append(jnp.dot(piece, gate_proj, preferred_element_type=F32).astype(BF16))
    for i, count in enumerate(parts):
        before = rim if i == 0 else (raw_x[i - 1][-keep:], raw_bc[i - 1][-keep:])
        x_all = conv_silu(join([before[0], raw_x[i]]), count * BLOCK, conv_weight, conv_bias)
        bc_all = conv_silu(join([before[1], raw_bc[i]]), count * BLOCK, bc_conv_weight, bc_conv_bias)
        for k in range(count):
            rows_k = slice(k * BLOCK, (k + 1) * BLOCK)
            x, bc = x_all[rows_k], bc_all[rows_k]
            b, c = bc[:, :n], bc[:, n:]
            y, u, cum, local, total = ssd_chunk(
                x, b, c, steps[i][rows_k], rate, skip_row, local, total, width
            )
            ys.append(y)
            us.append(u)
            cums.append(cum)
            cs.append(c)
    incoming = incoming_state(local, total)
    scale = QMAX / jnp.max(amax_history)
    out_parts = OUT_PARTS if sum(OUT_PARTS) == blocks else (1,) * blocks
    gain_row = norm_gain[None]
    quants, peak = gate_norm(
        ys, gates, cs, cums, us, incoming, gain_row, gain_row * scale, out_parts, width
    )
    results = []
    for part, quant in enumerate(quants):
        share = out_part(quant, out_proj, places)
        if part == len(out_parts) - 1:
            share, peak = lax.optimization_barrier((share, peak))
        summed = lax.psum_scatter(share, "tp", scatter_dimension=0, tiled=False)
        results.append((summed.astype(F32) / scale).astype(BF16))
    peak = lax.pmax(peak, ("seq", "tp"))
    mixed = join(results)
    return (mixed, jnp.concatenate([jnp.reshape(peak, (1,)), amax_history[:-1]]))


def solution(mesh):
    return jax.shard_map(
        shards,
        mesh=mesh,
        in_specs=(
            P("seq", "tp"), P(None, "tp"), P(None, "tp"), P(), P(None, "tp"), P("tp"), P("tp"), P(None, "tp"),
            P("tp"), P(), P(), P("tp"), P("tp"), P("tp", None), P(),
        ),
        out_specs=(P("seq", "tp"), P()),
        check_vma=False,
    )
```
